32 devices in a mesh: kgrp: 4 (over x, core), tile: 8 (over z, y).
Axes of the slice: x: 2, y: 2, z: 4, core: 2. Of those that a mesh axis runs over, the one named last changes fastest.
Arguments:
- mask_spectrum: float32 [32, 2, 512, 512], P(('kgrp', 'tile')), may hold values from -6 to 6
- kernels: float32 [8, 2, 512, 512], P('kgrp', None, 'tile'), may hold values from -6 to 6
- owner_table: int32 [4], replicated, may hold values from 0 to 7
- step_weight: float32 [4], replicated, may hold values from 0.25 to 1
Outputs:
- intensity: float32 [32, 512, 512], P(('kgrp', 'tile'))
The draws below stay inside these ranges and needn't reach their ends.
Inputs may be any that keep to these rules, and one draw needn't show every extreme that they name: `owner_table`: kernel indices, possibly repeated across steps.
All inputs are finite; a program needn't handle non-finite values.
Results may differ from the reference program's by a relative error of at most 0.0001.
Values sent between devices are 32-bit elements; how exact they have to be, the bound alone decides.
No kernel may reach another device: no remote copies, remote signals or barrier semaphores. Data moves between devices by JAX's collectives and lax.ppermute only.
A program may use at most 128 MiB of HBM per device.

```python
import math
import jax
import jax.numpy as jnp

KS = 512
STEPS = 4
KERNELS = 8
TILES = 32


def with_ends(entries, rng, least, high):
    longest = entries.shape.index(max(entries.shape))
    spots = []
    for shift in (0, 1):
        where = [jax.random.randint(jax.random.fold_in(rng, axis), (), 0, length) for axis, length in enumerate(entries.shape)]
        where[longest] = (where[longest] + shift) % entries.shape[longest]
        spots.append(tuple(where))
    return entries.at[spots[0]].set(least).at[spots[1]].set(high)


def shard_levels(rng, shape, cuts, least, largest):
    level = 1.0
    for position, parts in cuts:
        draws = jax.random.uniform(jax.random.fold_in(jax.random.fold_in(rng, 6), position), (parts,), jnp.float32, least / len(cuts), largest / len(cuts))
        level = level * jnp.repeat(jnp.exp(draws), shape[position] // parts).reshape((-1,) + (1,) * (len(shape) - 1 - position))
    return level


def bell_draw(own_key, shape, deviation, reach, pieces=(), kind=jnp.bfloat16):
    entries = deviation * jax.random.normal(own_key, shape, jnp.float32)
    if pieces:
        entries = entries * shard_levels(own_key, shape, pieces, -0.22, 0.18)
    return jnp.clip(entries, -reach, reach).astype(kind)


def setup_inputs(seed: int = 0) -> dict:
    key_of = jax.random.split(jax.random.key(seed), 5)
    mask_spectrum = bell_draw(key_of[0], (TILES, 2, KS, KS), 0.7, 6.0, ((0, 32),), jnp.float32)
    kernels = bell_draw(key_of[1], (KERNELS, 2, KS, KS), 0.7, 6.0, ((0, 4), (2, 8)), jnp.float32)
    owner_table = with_ends(jax.random.randint(key_of[2], (STEPS,), 0, KERNELS), jax.random.fold_in(key_of[2], 1), 0, KERNELS - 1).astype(jnp.int32)
    step_weight = jnp.clip(jnp.exp(jax.random.uniform(key_of[3], (STEPS,), jnp.float32, math.log(0.25), math.log(1.0))), 0.25, 1.0)
    return {"mask_spectrum": mask_spectrum, "kernels": kernels, "owner_table": owner_table, "step_weight": step_weight}


def reference(mask_spectrum, kernels, owner_table, step_weight):
    mask_field = mask_spectrum[:, 0] + 1j * mask_spectrum[:, 1]
    intensity = jnp.zeros_like(mask_spectrum[:, 0])
    for step in range(STEPS):
        kernel_pick = kernels[owner_table[step]]
        spectrum = mask_field * (kernel_pick[0] + 1j * kernel_pick[1])[None]
        aerial_field = jnp.fft.ifft2(spectrum, norm="ortho")
        power = jnp.real(aerial_field) ** 2 + jnp.imag(aerial_field) ** 2
        intensity = intensity + step_weight[step] * power.astype(intensity.dtype)
    return intensity
```

```python
import functools
import math

import jax
import jax.numpy as jnp
import numpy as np
from jax import lax
from jax.experimental import pallas as pl
from jax.experimental.pallas import tpu as pltpu
from jax.sharding import PartitionSpec as P


RADIX = 4
BF16 = jnp.bfloat16
F32 = jnp.float32

PIECES = (
    (((0, 0), (0, 1)), ("hlyx", "lyxh")),
    (((0, 2), (0, 3)), ("hxyl", "xlhy")),
    (((1, 0), (1, 1)), ("hlxy", "xyhl")),
    (((1, 2), (1, 3)), ("hlyx", "lhyx")),
)


def dft_tables(length):
    quarter = length // RADIX
    inner = np.arange(quarter)[:, None]
    tables = []
    for residue in range(RADIX):
        outer = RADIX * np.arange(quarter)[None, :] + residue
        angle = (inner * outer % length) * (2.0 * math.pi / length)
        cos, sin = np.cos(angle) / math.sqrt(length), np.sin(angle) / math.sqrt(length)
        tables.append(np.block([[cos, sin], [-sin, cos]]))
    table = np.stack(tables).astype(np.float32)
    high = table.astype(jnp.bfloat16)
    low = (table - high.astype(np.float32)).astype(jnp.bfloat16)
    right = np.stack([high, low])
    return right, np.ascontiguousarray(np.swapaxes(right, -1, -2))


def lane_order(length):
    quarter = length // RADIX
    table = np.zeros((length, length), np.float32)
    for lane in range(length):
        table[(lane % RADIX) * quarter + lane // RADIX, lane] = 1.0
    return table.astype(jnp.bfloat16)


def halves(value):
    high = value.astype(BF16)
    return high, (value - high.astype(F32)).astype(BF16)


def dot(left, right):
    return jnp.dot(left, right, preferred_element_type=F32)


def butterflies(quarters):
    (r0, i0), (r1, i1), (r2, i2), (r3, i3) = quarters
    sr, si, dr, di = r0 + r2, i0 + i2, r0 - r2, i0 - i2
    er, ei, fr, fi = r1 + r3, i1 + i3, r1 - r3, i1 - i3
    return (sr + er, si + ei), (dr - fi, di + fr), (sr - er, si - ei), (dr + fi, di - fr)


def unit_kernel(step, n_pieces, has_acc, length, sub, *refs):
    offs_ref, weight_ref, mask_ref, right_ref, left_ref = refs[:5]
    refs = refs[5:]
    piece_refs, refs = refs[: 2 * n_pieces], refs[2 * n_pieces :]
    if has_acc:
        acc_ref, refs = refs[0], refs[1:]
    out_ref, kern, rows_hi, rows_lo, z_ref, cols_hi, cols_lo, sem = refs
    quarter = length // RADIX

    def copies():
        index = 0
        for piece, (atoms, _) in enumerate(PIECES):
            if not any(a[0] == step for a in atoms):
                continue
            for part in range(2):
                ref = piece_refs[2 * index + part]
                for unit in range(ref.shape[0]):
                    offset = pl.multiple_of(offs_ref[piece, part * ref.shape[0] + unit], 8)
                    for slot, (s, q) in enumerate(atoms):
                        if s == step:
                            yield pltpu.make_async_copy(
                                ref.at[unit, slot],
                                kern.at[:, pl.ds(offset, sub), pl.ds(q * quarter, quarter)],
                                sem,
                            )
            index += 1

    for copy in copies():
        copy.start()
    pltpu.make_async_copy(kern, kern, sem).wait()

    block, chunk = 256, 32
    for base in range(0, length, block):

        @pl.loop(0, block // chunk)
        def _(i):
            at = pl.ds(pl.multiple_of(base + i * chunk, chunk), chunk)
            to = pl.ds(pl.multiple_of(i * chunk, chunk), chunk)
            quarters = []
            for j in range(RADIX):
                lanes = pl.ds(j * quarter, quarter)
                mr, mi = mask_ref[0, at, lanes], mask_ref[1, at, lanes]
                kr, ki = kern[0, at, lanes], kern[1, at, lanes]
                quarters.append((mr * kr - mi * ki, mr * ki + mi * kr))
            for r, (re, im) in enumerate(butterflies(quarters)):
                for part, value in enumerate((re, im)):
                    lanes = pl.ds(part * quarter, quarter)
                    rows_hi[r, to, lanes], rows_lo[r, to, lanes] = halves(value)

        for r in range(RADIX):
            z_ref[r, pl.ds(base, block), :] = (
                dot(rows_hi[r], right_ref[0, r])
                + dot(rows_lo[r], right_ref[0, r])
                + dot(rows_hi[r], right_ref[1, r])
            )

    for r in range(RADIX):

        @pl.loop(0, quarter // chunk)
        def _(i):
            at = pl.multiple_of(i * chunk, chunk)
            quarters = []
            for j in range(RADIX):
                rows = pl.ds(pl.multiple_of(j * quarter + at, chunk), chunk)
                quarters.append((z_ref[r, rows, :quarter], z_ref[r, rows, quarter:]))
            for rho, (re, im) in enumerate(butterflies(quarters)):
                for part, value in enumerate((re, im)):
                    rows = pl.ds(pl.multiple_of(part * quarter + at, chunk), chunk)
                    lanes = pl.ds(r * quarter, quarter)
                    cols_hi[rho, rows, lanes], cols_lo[rho, rows, lanes] = halves(value)

    weight = weight_ref[step]
    for rho in range(RADIX):
        for lanes in (pl.ds(0, length // 2), pl.ds(length // 2, length // 2)):
            field = (
                dot(left_ref[0, rho], cols_hi[rho, :, lanes])
                + dot(left_ref[1, rho], cols_hi[rho, :, lanes])
                + dot(left_ref[0, rho], cols_lo[rho, :, lanes])
            )
            re, im = field[:quarter], field[quarter:]
            value = weight * (re * re + im * im)
            if has_acc:
                value = value + acc_ref[rho, :, lanes]
            out_ref[rho, :, lanes] = value


def unit(step, mask, pieces, offs, weights, tables, acc=None):
    length = mask.shape[-1]
    used = [pair for pair, (atoms, _) in zip(pieces, PIECES) if any(a[0] == step for a in atoms)]
    sub = used[0][0].shape[-2]
    flat = [ref for pair in used for ref in pair]
    vmem, anyspace, smem = (
        pl.BlockSpec(memory_space=pltpu.VMEM),
        pl.BlockSpec(memory_space=pl.ANY),
        pl.BlockSpec(memory_space=pltpu.SMEM),
    )
    quarter = length // RADIX
    extra = [] if acc is None else [acc]
    return pl.pallas_call(
        functools.partial(unit_kernel, step, len(used), acc is not None, length, sub),
        out_shape=jax.ShapeDtypeStruct((RADIX, quarter, length), F32),
        in_specs=[smem, smem, vmem, vmem, vmem] + [anyspace] * len(flat) + [vmem] * len(extra),
        out_specs=vmem,
        scratch_shapes=[
            pltpu.VMEM((2, length, length), F32),
            pltpu.VMEM((RADIX, 256, 2 * quarter), BF16),
            pltpu.VMEM((RADIX, 256, 2 * quarter), BF16),
            pltpu.VMEM((RADIX, length, 2 * quarter), F32),
            pltpu.VMEM((RADIX, 2 * quarter, length), BF16),
            pltpu.VMEM((RADIX, 2 * quarter, length), BF16),
            pltpu.SemaphoreType.DMA,
        ],
        compiler_params=pltpu.CompilerParams(vmem_limit_bytes=40 * 2**20),
        cost_estimate=pl.CostEstimate(flops=3 * 2**30, bytes_accessed=8 * 2**20, transcendentals=0),
        name=f"unit{step}",
    )(offs, weights, mask, *tables, *flat, *extra)


def finish_kernel(a_ref, b_ref, order_ref, out_ref, split_ref):
    quarter = a_ref.shape[1]
    for rho in range(RADIX):
        high, low = halves(a_ref[rho] + b_ref[rho])
        value = dot(high, order_ref[...]) + dot(low, order_ref[...])
        for q in range(RADIX):
            split_ref[q, pl.ds(rho, quarter, stride=RADIX), :] = value[:, q * quarter : (q + 1) * quarter]
    for q in range(RADIX):
        out_ref[:, q * quarter : (q + 1) * quarter] = split_ref[q]


def finish(mine, other, order):
    _, quarter, length = mine.shape
    return pl.pallas_call(
        finish_kernel,
        out_shape=jax.ShapeDtypeStruct((length, length), F32),
        in_specs=[pl.BlockSpec(memory_space=pltpu.VMEM)] * 3,
        out_specs=pl.BlockSpec(memory_space=pltpu.VMEM),
        scratch_shapes=[pltpu.VMEM((RADIX, length, quarter), F32)],
        cost_estimate=pl.CostEstimate(flops=2**28, bytes_accessed=3 * 2**20, transcendentals=0),
        name="finish",
    )(mine, other, order)


def local(groups, tiles, mask_spectrum, kernels, owner_table, step_weight):
    own_mask = mask_spectrum[0]
    length = own_mask.shape[-1]
    slots, _, slab, _ = kernels.shape
    steps = owner_table.shape[0]
    per_core = steps // 2
    devices = groups * tiles
    sub = slab // (groups // 2)
    quarter = length // RADIX
    group, tile = lax.axis_index("kgrp"), lax.axis_index("tile")
    core, xpos = group % 2, group // 2
    me = group * tiles + tile

    core_bit, x_bit, y_bit, low_bit = tiles, 2 * tiles, 1, 2
    high_bits = [bit for bit in (2**k for k in range(2, 10)) if bit < tiles]
    bits = {"x": [x_bit], "y": [y_bit], "l": [low_bit], "h": high_bits}

    def exchange(value, flips):
        pairs = [(i, i ^ flips[(i // tiles) % 2]) for i in range(devices)]
        return lax.ppermute(value, ("kgrp", "tile"), pairs)

    other_mask = exchange(own_mask, (core_bit, core_bit))

    owner_group, owner_slot = owner_table // slots, owner_table % slots

    def chosen(which):
        index = lax.dynamic_slice_in_dim(owner_slot, which * per_core, per_core)
        return jnp.stack([lax.dynamic_index_in_dim(kernels, index[s], 0, False) for s in range(per_core)])

    def wide(flags):
        return flags[:, None, None, None]

    owners = lax.dynamic_slice_in_dim(owner_group, core * per_core, per_core)
    received = exchange(chosen(1 - core), (core_bit, core_bit))
    chip = jnp.where(wide(owners == group), chosen(core), received)
    keep = lax.dynamic_slice_in_dim(chip, xpos * sub, sub, 2)
    give = lax.dynamic_slice_in_dim(chip, (1 - xpos) * sub, sub, 2)
    received = exchange(give, (x_bit, x_bit))
    mine = jnp.where(wide(owners // 2 == xpos), keep, received)

    pieces, offsets, current, orders = [], [], [], []
    for atoms, order in PIECES:
        value = jnp.stack([mine[s, :, :, q * quarter : (q + 1) * quarter] for s, q in atoms])
        current.append(value[None])
        orders.append([[bit for letter in o for bit in bits[letter]] for o in order])
    rounds = len(orders[0][0])
    for r in range(rounds):
        for i in range(len(PIECES)):
            got = exchange(current[i], (orders[i][0][r], orders[i][1][r]))
            if r < rounds - 1:
                current[i] = jnp.concatenate([current[i], got])
            else:
                pieces.append((current[i], got))
    for order in orders:
        origin = []
        for which in range(2):
            flips = [0]
            for bit in order[which]:
                flips = flips + [f ^ bit for f in flips]
            origin.append(np.array(flips, np.int32))
        source = me ^ jnp.where(core == 0, origin[0], origin[1])
        offsets.append((source % tiles) * slab + (source // x_bit) * sub)
    offs = jnp.stack(offsets).astype(jnp.int32)
    weights = lax.dynamic_slice_in_dim(step_weight, core * per_core, per_core)

    right, left = dft_tables(length)
    tables = (jnp.asarray(right), jnp.asarray(left))
    args = (offs, weights, tables)
    theirs = unit(0, other_mask, pieces, *args)
    ours = unit(0, own_mask, pieces, *args)
    theirs = unit(1, other_mask, pieces, *args, acc=theirs)
    arrived = exchange(theirs, (core_bit, core_bit))
    ours = unit(1, own_mask, pieces, *args, acc=ours)
    return finish(ours, arrived, jnp.asarray(lane_order(length)))[None]


def solution(mesh):
    in_specs = (P(("kgrp", "tile"), None, None, None), P("kgrp", None, "tile", None), P(), P())
    out_specs = P(("kgrp", "tile"), None, None)
    body = functools.partial(local, mesh.shape["kgrp"], mesh.shape["tile"])
    return jax.shard_map(body, mesh=mesh, in_specs=in_specs, out_specs=out_specs, check_vma=False)
```

```python
import functools
import math

import jax
import jax.numpy as jnp
import numpy as np
from jax import lax
from jax.experimental import pallas as pl
from jax.experimental.pallas import tpu as pltpu
from jax.sharding import PartitionSpec as P


RADIX = 4
BF16 = jnp.bfloat16
F32 = jnp.float32

PIECES = (
    (((0, 0), (0, 1)), ("lhyx", "hlxy")),
    (((0, 2), (0, 3)), ("hxly", "lyhx")),
    (((1, 0), (1, 1)), ("hylx", "hxly")),
    (((1, 2), (1, 3)), ("xlyh", "yhxl")),
)


def dft_tables(length):
    quarter = length // RADIX
    inner = np.arange(quarter)[:, None]
    tables = []
    for residue in range(RADIX):
        outer = RADIX * np.arange(quarter)[None, :] + residue
        angle = (inner * outer % length) * (2.0 * math.pi / length)
        cos, sin = np.cos(angle) / math.sqrt(length), np.sin(angle) / math.sqrt(length)
        tables.append(np.block([[cos, sin], [-sin, cos]]))
    table = np.stack(tables).astype(np.float32)
    high = table.astype(jnp.bfloat16)
    low = (table - high.astype(np.float32)).astype(jnp.bfloat16)
    right = np.stack([high, low])
    left = np.concatenate([np.swapaxes(high, -1, -2), np.swapaxes(low, -1, -2)], axis=1)
    return right, np.ascontiguousarray(left)


def lane_order(length):
    quarter = length // RADIX
    row = lax.broadcasted_iota(jnp.int32, (length, length), 0)
    lane = lax.broadcasted_iota(jnp.int32, (length, length), 1)
    return (row == (lane % RADIX) * quarter + lane // RADIX).astype(BF16)


def halves(value):
    high = value.astype(BF16)
    return high, (value - high.astype(F32)).astype(BF16)


def dot(left, right):
    return jnp.dot(left, right, preferred_element_type=F32)


def butterflies(quarters):
    (r0, i0), (r1, i1), (r2, i2), (r3, i3) = quarters
    sr, si, dr, di = r0 + r2, i0 + i2, r0 - r2, i0 - i2
    er, ei, fr, fi = r1 + r3, i1 + i3, r1 - r3, i1 - i3
    return (sr + er, si + ei), (dr - fi, di + fr), (sr - er, si - ei), (dr + fi, di - fr)


def unit_kernel(step, origins, tiles, per_core, n_pieces, n_tiles, has_acc, length, sub, *refs):
    weight_ref, right_ref, left_ref = refs[:3]
    mask_refs, refs = refs[3 : 3 + n_tiles], refs[3 + n_tiles :]
    piece_refs, refs = refs[: 2 * n_pieces], refs[2 * n_pieces :]
    acc_refs, refs = (refs[:n_tiles], refs[n_tiles:]) if has_acc else ((None,) * n_tiles, refs)
    out_refs, refs = refs[:n_tiles], refs[n_tiles:]
    kern, rows, z_ref, cols_hi, cols_lo, sem = refs
    quarter = length // RADIX

    group = lax.axis_index("kgrp")
    core = lax.rem(group, 2)
    me = group * tiles + lax.axis_index("tile")
    slab = length // tiles
    index = 0
    for piece, (atoms, _) in enumerate(PIECES):
        if not any(a[0] == step for a in atoms):
            continue
        for part in range(2):
            ref = piece_refs[2 * index + part]
            for unit in range(ref.shape[0]):
                flips = [origins[piece][which][part * ref.shape[0] + unit] for which in range(2)]
                source = jnp.bitwise_xor(me, jnp.where(core == 0, flips[0], flips[1]))
                offset = pl.multiple_of(lax.rem(source, tiles) * slab + source // (2 * tiles) * sub, 8)
                for slot, (s, q) in enumerate(atoms):
                    if s == step:
                        to = kern.at[:, pl.ds(offset, sub), pl.ds(q * quarter, quarter)]
                        pltpu.make_async_copy(ref.at[unit, slot], to, sem).start()
        index += 1
    pltpu.make_async_copy(kern, kern, sem).wait()

    block, chunk = 128, 16

    def fill_rows(tile, b):
        for base in range(0, block, chunk):
            at = pl.ds(b * block + base, chunk)
            quarters = []
            for j in range(RADIX):
                lanes = pl.ds(j * quarter, quarter)
                mr, mi = mask_refs[tile][0, at, lanes], mask_refs[tile][1, at, lanes]
                kr, ki = kern[0, at, lanes], kern[1, at, lanes]
                quarters.append((mr * kr - mi * ki, mr * ki + mi * kr))
            for r, pair in enumerate(butterflies(quarters)):
                for part, value in enumerate(pair):
                    high, low = halves(value)
                    lanes = pl.ds(part * quarter, quarter)
                    rows[b % 2, r, pl.ds(base, chunk), lanes] = high
                    rows[b % 2, r, pl.ds(block + base, chunk), lanes] = low

    def along_rows(b):
        for r in range(RADIX):
            both = dot(rows[b % 2, r], right_ref[0, r])
            rest = dot(rows[b % 2, r, :block], right_ref[1, r])
            z_ref[r, pl.ds(b * block, block), :] = both[:block] + both[block:] + rest

    def fill_cols(r):
        for base in range(0, quarter, chunk):
            quarters = []
            for j in range(RADIX):
                at = pl.ds(j * quarter + base, chunk)
                quarters.append((z_ref[r, at, :quarter], z_ref[r, at, quarter:]))
            for rho, pair in enumerate(butterflies(quarters)):
                for part, value in enumerate(pair):
                    at, lanes = pl.ds(part * quarter + base, chunk), pl.ds(r * quarter, quarter)
                    cols_hi[rho, at, lanes], cols_lo[rho, at, lanes] = halves(value)

    weight = weight_ref[core * per_core + step]

    def along_cols(tile, pair):
        lanes = pl.ds(pair * 2 * quarter, 2 * quarter)
        for rho in range(RADIX):
            both = dot(left_ref[rho], cols_hi[rho, :, lanes])
            rest = dot(left_ref[rho, : 2 * quarter], cols_lo[rho, :, lanes])
            field = both[: 2 * quarter] + both[2 * quarter :] + rest
            re, im = field[:quarter], field[quarter:]
            value = weight * (re * re + im * im)
            if has_acc:
                value = value + acc_refs[tile][rho, :, lanes]
            out_refs[tile][rho, :, lanes] = value

    blocks = length // block
    for tile in range(n_tiles):
        fill_rows(tile, 0)
        for b in range(blocks):
            if b + 1 < blocks:
                fill_rows(tile, b + 1)
            along_rows(b)
        fill_cols(0)
        fill_cols(1)
        along_cols(tile, 0)
        fill_cols(2)
        fill_cols(3)
        along_cols(tile, 1)


def unit(step, masks, pieces, origins, tiles, weights, tables, accs=()):
    length = masks[0].shape[-1]
    used = [pair for pair, (atoms, _) in zip(pieces, PIECES) if any(a[0] == step for a in atoms)]
    sub = used[0][0].shape[-2]
    flat = [ref for pair in used for ref in pair]
    quarter = length // RADIX
    vmem = pl.BlockSpec(memory_space=pltpu.VMEM)
    anyspace = pl.BlockSpec(memory_space=pltpu.HBM)
    smem = pl.BlockSpec(memory_space=pltpu.SMEM)
    n = len(masks)
    return pl.pallas_call(
        functools.partial(
            unit_kernel, step, origins, tiles, weights.shape[0] // 2, len(used), n, bool(accs), length, sub
        ),
        out_shape=[jax.ShapeDtypeStruct((RADIX, quarter, length), F32)] * n,
        in_specs=[smem, vmem, vmem] + [vmem] * n + [anyspace] * len(flat) + [vmem] * len(accs),
        out_specs=[vmem] * n,
        scratch_shapes=[
            pltpu.VMEM((2, length, length), F32),
            pltpu.VMEM((2, RADIX, 256, 2 * quarter), BF16),
            pltpu.VMEM((RADIX, length, 2 * quarter), F32),
            pltpu.VMEM((RADIX, 2 * quarter, length), BF16),
            pltpu.VMEM((RADIX, 2 * quarter, length), BF16),
            pltpu.SemaphoreType.DMA,
        ],
        compiler_params=pltpu.CompilerParams(vmem_limit_bytes=12 * 2**20),
        cost_estimate=pl.CostEstimate(flops=n * 3 * 2**30, bytes_accessed=8 * 2**20, transcendentals=0),
        name=f"unit{step}x{n}",
    )(weights, *tables, *masks, *flat, *accs)


def resolve_kernel(slots, owner_ref, mine_ref, other_ref, *out_refs):
    group = lax.axis_index("kgrp")
    core, xpos = lax.rem(group, 2), group // 2
    per_core = len(out_refs) // 3
    sub = out_refs[0].shape[1]
    for step in range(per_core):
        kernel = owner_ref[core * per_core + step]
        owner, slot = kernel // slots, lax.rem(kernel, slots)
        here = jnp.where(owner // 2 == xpos, 1.0, 0.0)
        out_refs[2 * per_core + step][...] = jnp.full(out_refs[2 * per_core + step].shape, here, F32)
        for source, wanted in ((mine_ref, lax.rem(owner, 2) == core), (other_ref, lax.rem(owner, 2) != core)):

            @pl.when(wanted)
            def _():
                for place, half in ((0, 1 - xpos), (1, xpos)):
                    at = pl.ds(pl.multiple_of(half * sub, 8), sub)
                    out_refs[2 * step + place][...] = source[slot, :, at, :]


def resolve(owner_table, mine, other, per_core, sub):
    slots, parts, _, length = mine.shape
    vmem = pl.BlockSpec(memory_space=pltpu.VMEM)
    return pl.pallas_call(
        functools.partial(resolve_kernel, slots),
        out_shape=[jax.ShapeDtypeStruct((parts, sub, length), F32)] * (2 * per_core)
        + [jax.ShapeDtypeStruct((sub, length), F32)] * per_core,
        in_specs=[pl.BlockSpec(memory_space=pltpu.SMEM), vmem, vmem],
        out_specs=[vmem] * (3 * per_core),
        compiler_params=pltpu.CompilerParams(vmem_limit_bytes=4 * 2**20),
        name="resolve",
    )(owner_table, mine, other)


def finish_kernel(a_ref, b_ref, order_ref, out_ref, both, split):
    quarter, length = a_ref.shape[1:]
    for rho in range(RADIX):
        high, low = halves(a_ref[rho] + b_ref[rho])
        both[0, pl.ds(rho * quarter, quarter), :] = high
        both[1, pl.ds(rho * quarter, quarter), :] = low
    for q in range(0, RADIX, 2):
        lanes = slice(q * quarter, (q + 2) * quarter)
        value = dot(both[0], order_ref[:, lanes]) + dot(both[1], order_ref[:, lanes])
        for rho in range(RADIX):
            rows = slice(rho * quarter, (rho + 1) * quarter)
            for k in range(2):
                split[q + k, pl.ds(rho, quarter, stride=RADIX), :] = value[rows, k * quarter : (k + 1) * quarter]
        for k in range(2):
            out_ref[:, (q + k) * quarter : (q + k + 1) * quarter] = split[q + k]


def finish(mine, other, order):
    _, quarter, length = mine.shape
    vmem = pl.BlockSpec(memory_space=pltpu.VMEM)
    return pl.pallas_call(
        finish_kernel,
        out_shape=jax.ShapeDtypeStruct((length, length), F32),
        in_specs=[vmem] * 3,
        out_specs=vmem,
        scratch_shapes=[pltpu.VMEM((2, length, length), BF16), pltpu.VMEM((RADIX, length, quarter), F32)],
        compiler_params=pltpu.CompilerParams(vmem_limit_bytes=8 * 2**20),
        cost_estimate=pl.CostEstimate(flops=2**28, bytes_accessed=3 * 2**20, transcendentals=0),
        name="finish",
    )(mine, other, order)


def local(groups, tiles, mask_spectrum, kernels, owner_table, step_weight):
    own_mask = mask_spectrum[0]
    length = own_mask.shape[-1]
    slots, _, slab, _ = kernels.shape
    steps = owner_table.shape[0]
    per_core = steps // 2
    devices = groups * tiles
    sub = slab // (groups // 2)
    quarter = length // RADIX

    core_bit, x_bit, y_bit, low_bit = tiles, 2 * tiles, 1, 2
    high_bits = [bit for bit in (2**k for k in range(2, 10)) if bit < tiles]
    bits = {"x": [x_bit], "y": [y_bit], "l": [low_bit], "h": high_bits}

    def exchange(value, flips):
        pairs = [(i, i ^ flips[(i // tiles) % 2]) for i in range(devices)]
        return lax.ppermute(value, ("kgrp", "tile"), pairs)

    received = exchange(kernels, (core_bit, core_bit))
    other_mask = exchange(own_mask, (core_bit, core_bit))
    parted = resolve(owner_table, kernels, received, per_core, sub)
    values = []
    for step in range(per_core):
        give, keep = parted[2 * step : 2 * step + 2]
        got = exchange(give, (x_bit, x_bit))
        values.append(jnp.where(parted[2 * per_core + step][None] > 0.5, keep, got))

    pieces, origins, current, orders = [], [], [], []
    for atoms, order in PIECES:
        value = jnp.stack([values[s][:, :, q * quarter : (q + 1) * quarter] for s, q in atoms])
        current.append(value[None])
        orders.append([[bit for letter in o for bit in bits[letter]] for o in order])
    rounds = len(orders[0][0])
    for r in range(rounds):
        for i in range(len(PIECES)):
            got = exchange(current[i], (orders[i][0][r], orders[i][1][r]))
            if r < rounds - 1:
                current[i] = jnp.concatenate([current[i], got])
            else:
                pieces.append((current[i], got))
    for order in orders:
        origin = []
        for which in range(2):
            flips = [0]
            for bit in order[which]:
                flips = flips + [f ^ bit for f in flips]
            origin.append(flips)
        origins.append(origin)

    right, left = dft_tables(length)
    tables = (jnp.asarray(right), jnp.asarray(left))
    args = (origins, tiles, step_weight, tables)
    theirs, ours = unit(0, [other_mask, own_mask], pieces, *args)
    (theirs,) = unit(1, [other_mask], pieces, *args, accs=[theirs])
    arrived = exchange(theirs, (core_bit, core_bit))
    (ours,) = unit(1, [own_mask], pieces, *args, accs=[ours])
    return finish(ours, arrived, lane_order(length))[None]


def solution(mesh):
    in_specs = (P(("kgrp", "tile"), None, None, None), P("kgrp", None, "tile", None), P(), P())
    out_specs = P(("kgrp", "tile"), None, None)
    body = functools.partial(local, mesh.shape["kgrp"], mesh.shape["tile"])
    return jax.shard_map(body, mesh=mesh, in_specs=in_specs, out_specs=out_specs, check_vma=False)
```

```python
import functools
import itertools
import math

import jax
import jax.numpy as jnp
import numpy as np
from jax import lax
from jax.experimental import pallas as pl
from jax.experimental.pallas import tpu as pltpu
from jax.sharding import PartitionSpec as P


RADIX = 4
BF16 = jnp.bfloat16
F32 = jnp.float32

PIECES = (
    ((0, 0, 2), ("lhyx", "hlxy")),
    ((0, 2, 2), ("lhxy", "hyxl")),
    ((1, 0, 2), ("hlyx", "xyhl")),
    ((1, 2, 2), ("hlxy", "xyhl")),
)
SHARED = (1, 2)


def dft_tables(length):
    quarter = length // RADIX
    inner = np.arange(quarter)[:, None]
    tables = []
    for residue in range(RADIX):
        outer = RADIX * np.arange(quarter)[None, :] + residue
        angle = (inner * outer % length) * (2.0 * math.pi / length)
        cos, sin = np.cos(angle) / math.sqrt(length), np.sin(angle) / math.sqrt(length)
        tables.append(np.block([[cos, sin], [-sin, cos]]))
    table = np.stack(tables).astype(np.float32)
    high = table.astype(jnp.bfloat16)
    low = (table - high.astype(np.float32)).astype(jnp.bfloat16)
    right = np.stack([high, low])
    left = np.concatenate([np.swapaxes(high, -1, -2), np.swapaxes(low, -1, -2)], axis=1)
    return right, np.ascontiguousarray(left)


def lane_order(length):
    quarter = length // RADIX
    row = lax.broadcasted_iota(jnp.int32, (length, length), 0)
    lane = lax.broadcasted_iota(jnp.int32, (length, length), 1)
    return (row == (lane % RADIX) * quarter + lane // RADIX).astype(BF16)


def halves(value):
    high = value.astype(BF16)
    return high, (value - high.astype(F32)).astype(BF16)


def dot(left, right):
    return jnp.dot(left, right, preferred_element_type=F32)


def butterflies(quarters):
    (r0, i0), (r1, i1), (r2, i2), (r3, i3) = quarters
    sr, si, dr, di = r0 + r2, i0 + i2, r0 - r2, i0 - i2
    er, ei, fr, fi = r1 + r3, i1 + i3, r1 - r3, i1 - i3
    return (sr + er, si + ei), (dr - fi, di + fr), (sr - er, si - ei), (dr + fi, di - fr)


def unit_kernel(step, origins, tiles, per_core, n_pieces, n_tiles, has_acc, keep, length, *refs):
    weight_ref, right_ref, left_ref = refs[:3]
    mask_refs, refs = refs[3 : 3 + n_tiles], refs[3 + n_tiles :]
    piece_refs, refs = refs[: 2 * n_pieces], refs[2 * n_pieces :]
    acc_refs, refs = (refs[:n_tiles], refs[n_tiles:]) if has_acc else ((None,) * n_tiles, refs)
    if not n_pieces:
        kern, refs = refs[0], refs[1:]
    out_refs, refs = refs[:n_tiles], refs[n_tiles:]
    if n_pieces:
        kern, refs = refs[0], refs[1:]
    rows, z_ref, cols_hi, cols_lo, sem = refs
    quarter = length // RADIX

    group = lax.axis_index("kgrp")
    core = lax.rem(group, 2)
    me = group * tiles + lax.axis_index("tile")
    slab = length // tiles
    index = 0
    for piece, ((piece_step, first, count), _) in enumerate(PIECES):
        if not n_pieces or piece_step != step:
            continue
        sub = piece_refs[0].shape[-2]
        for part in range(2):
            ref = piece_refs[2 * index + part]
            for unit in range(ref.shape[0]):
                flips = [origins[piece][which][part * ref.shape[0] + unit] for which in range(2)]
                flip = flips[0] if flips[0] == flips[1] else jnp.where(core == 0, flips[0], flips[1])
                source = jnp.bitwise_xor(me, flip)
                row = jnp.bitwise_and(source, tiles - 1) * slab
                row = row + lax.shift_right_logical(source, (2 * tiles).bit_length() - 1) * sub
                to = kern.at[:, pl.ds(pl.multiple_of(row, 8), sub), pl.ds(first * quarter, count * quarter)]
                pltpu.make_async_copy(ref.at[unit], to, sem).start()
        index += 1
    if n_pieces:
        pltpu.make_async_copy(kern, kern, sem).wait()

    block, chunk = 128, 16
    slots = rows.shape[0]
    weight = weight_ref[core * per_core + step]

    def fill_rows(tile, b, base):
        at = pl.ds(b * block + base, chunk)
        quarters = []
        for j in range(RADIX):
            lanes = pl.ds(j * quarter, quarter)
            mr, mi = mask_refs[tile][0, at, lanes], mask_refs[tile][1, at, lanes]
            kr, ki = kern[0, at, lanes], kern[1, at, lanes]
            quarters.append((mr * kr - mi * ki, mr * ki + mi * kr))
        for r, pair in enumerate(butterflies(quarters)):
            for part, value in enumerate(pair):
                high, low = halves(value)
                lanes = pl.ds(part * quarter, quarter)
                rows[b % slots, r, pl.ds(base, chunk), lanes] = high
                rows[b % slots, r, pl.ds(block + base, chunk), lanes] = low

    def along_rows(b, r):
        both = dot(rows[b % slots, r], right_ref[0, r])
        rest = dot(rows[b % slots, r, :block], right_ref[1, r])
        z_ref[r, pl.ds(b * block, block), :] = both[:block] + both[block:] + rest

    def fill_cols(r, base):
        quarters = []
        for j in range(RADIX):
            at = pl.ds(j * quarter + base, chunk)
            quarters.append((z_ref[r, at, :quarter], z_ref[r, at, quarter:]))
        for rho, pair in enumerate(butterflies(quarters)):
            for part, value in enumerate(pair):
                at, lanes = pl.ds(part * quarter + base, chunk), pl.ds(r * quarter, quarter)
                cols_hi[rho, at, lanes], cols_lo[rho, at, lanes] = halves(value)

    def along_cols(tile, pair, rho):
        lanes = pl.ds(pair * 2 * quarter, 2 * quarter)
        both = dot(left_ref[rho], cols_hi[rho, :, lanes])
        rest = dot(left_ref[rho, : 2 * quarter], cols_lo[rho, :, lanes])
        field = both[: 2 * quarter] + both[2 * quarter :] + rest
        re, im = field[:quarter], field[quarter:]
        value = weight * (re * re + im * im)
        if has_acc:
            value = value + acc_refs[tile][rho, :, lanes]
        out_refs[tile][rho, :, lanes] = value

    def tasks(function, *lists):
        return [functools.partial(function, *args) for args in itertools.product(*lists)]

    def mix(matmuls, fills):
        count = max(len(matmuls), 1)
        for index in range(count):
            for task in matmuls[index : index + 1]:
                task()
            for task in fills[index * len(fills) // count : (index + 1) * len(fills) // count]:
                task()

    bases, quads = range(0, block, chunk), range(RADIX)
    blocks = range(length // block)
    ahead = range(0, quarter, chunk)
    now, later = (quads[:2], quads[2:]) if slots == len(blocks) else (quads, ())
    mix([], tasks(fill_rows, [0], [0], bases))
    for tile in range(n_tiles):
        for b in blocks[:-1]:
            mix(tasks(along_rows, [b], now), tasks(fill_rows, [tile], [b + 1], bases))
        mix(tasks(along_rows, blocks[-1:], now), [])
        mix(tasks(along_rows, blocks, later), tasks(fill_cols, [0, 1], ahead))
        mix(tasks(along_cols, [tile], [0], quads), tasks(fill_cols, [2, 3], ahead))
        following = tasks(fill_rows, [tile + 1], [0], bases) if tile + 1 < n_tiles else []
        mix(tasks(along_cols, [tile], [1], quads), following)


def unit(step, masks, pieces, origins, tiles, weights, tables, accs=(), kern=None, keep=False):
    length = masks[0].shape[-1]
    used = [pair for pair, (part, _) in zip(pieces, PIECES) if kern is None and part[0] == step]
    flat = [ref for pair in used for ref in pair]
    quarter = length // RADIX
    vmem = pl.BlockSpec(memory_space=pltpu.VMEM)
    hbm = pl.BlockSpec(memory_space=pltpu.HBM)
    smem = pl.BlockSpec(memory_space=pltpu.SMEM)
    n = len(masks)
    late = list(accs) + ([] if kern is None else [kern])
    whole = jax.ShapeDtypeStruct((2, length, length), F32)
    scratch = [
        pltpu.VMEM((2 if n > 1 else length // 128, RADIX, 256, 2 * quarter), BF16),
        pltpu.VMEM((RADIX, length, 2 * quarter), F32),
        pltpu.VMEM((RADIX, 2 * quarter, length), BF16),
        pltpu.VMEM((RADIX, 2 * quarter, length), BF16),
        pltpu.SemaphoreType.DMA,
    ]
    if used and not keep:
        scratch = [pltpu.VMEM(whole.shape, F32)] + scratch
    return pl.pallas_call(
        functools.partial(
            unit_kernel, step, origins, tiles, weights.shape[0] // 2, len(used), n, bool(accs), keep, length
        ),
        out_shape=[jax.ShapeDtypeStruct((RADIX, quarter, length), F32)] * n + [whole] * keep,
        in_specs=[smem, vmem, vmem] + [vmem] * n + [hbm] * len(flat) + [vmem] * len(late),
        out_specs=[vmem] * (n + keep),
        scratch_shapes=scratch,
        compiler_params=pltpu.CompilerParams(vmem_limit_bytes=12 * 2**20),
        cost_estimate=pl.CostEstimate(flops=n * 3 * 2**30, bytes_accessed=8 * 2**20, transcendentals=0),
    )(weights, *tables, *masks, *flat, *late)


def stage_kernel(per_core, owner_ref, kernels_ref, local_ref, flags_ref, *here_refs):
    slots = kernels_ref.shape[0]
    group = lax.axis_index("kgrp")
    core, xpos = lax.rem(group, 2), group // 2
    flags = [xpos == 1]
    for step in range(per_core):
        kernel = owner_ref[core * per_core + step]
        owner, slot = kernel // slots, lax.rem(kernel, slots)
        local_ref[step] = kernels_ref[slot]
        flags += [lax.rem(owner, 2) == core] + [slot == j for j in range(1, slots)]
        here = jnp.where(owner // 2 == xpos, 1.0, 0.0)
        here_refs[step][...] = jnp.full(here_refs[step].shape, here, F32)
    for row, flag in enumerate(flags):
        flags_ref[row] = jnp.full(flags_ref.shape[1:], jnp.where(flag, 1.0, 0.0), F32)


def stage(owner_table, kernels, per_core):
    slots, parts, slab, length = kernels.shape
    vmem = pl.BlockSpec(memory_space=pltpu.VMEM)
    return pl.pallas_call(
        functools.partial(stage_kernel, per_core),
        out_shape=[
            jax.ShapeDtypeStruct((per_core, parts, slab, length), F32),
            jax.ShapeDtypeStruct((1 + per_core * slots, 8, length), F32),
        ]
        + [jax.ShapeDtypeStruct((8, length), F32)] * per_core,
        in_specs=[pl.BlockSpec(memory_space=pltpu.SMEM), vmem],
        out_specs=[vmem] * (2 + per_core),
        compiler_params=pltpu.CompilerParams(vmem_limit_bytes=4 * 2**20),
        name="stage",
    )(owner_table, kernels)


def finish_kernel(a_ref, b_ref, order_ref, out_ref, both, split, sem):
    quarter, _ = a_ref.shape[1:]
    for rho in range(RADIX):
        high, low = halves(a_ref[rho] + b_ref[rho])
        both[0, pl.ds(rho * quarter, quarter), :] = high
        both[1, pl.ds(rho * quarter, quarter), :] = low
    copies = []
    for q in range(0, RADIX, 2):
        lanes = slice(q * quarter, (q + 2) * quarter)
        value = dot(both[0], order_ref[:, lanes]) + dot(both[1], order_ref[:, lanes])
        for k in range(2):
            for rho in range(RADIX):
                rows = slice(rho * quarter, (rho + 1) * quarter)
                split[q + k, pl.ds(rho, quarter, stride=RADIX), :] = value[rows, k * quarter : (k + 1) * quarter]
            to = out_ref.at[:, pl.ds((q + k) * quarter, quarter)]
            copies.append(pltpu.make_async_copy(split.at[q + k], to, sem.at[q + k]))
            copies[-1].start()
    for copy in copies:
        copy.wait()


def finish(mine, other, order):
    _, quarter, length = mine.shape
    vmem = pl.BlockSpec(memory_space=pltpu.VMEM)
    return pl.pallas_call(
        finish_kernel,
        out_shape=jax.ShapeDtypeStruct((length, length), F32),
        in_specs=[vmem] * 3,
        out_specs=pl.BlockSpec(memory_space=pltpu.HBM),
        scratch_shapes=[
            pltpu.VMEM((2, length, length), BF16),
            pltpu.VMEM((RADIX, length, quarter), F32),
            pltpu.SemaphoreType.DMA((RADIX,)),
        ],
        compiler_params=pltpu.CompilerParams(vmem_limit_bytes=8 * 2**20),
        cost_estimate=pl.CostEstimate(flops=2**28, bytes_accessed=3 * 2**20, transcendentals=0),
        name="finish",
    )(mine, other, order)


def local(groups, tiles, mask_spectrum, kernels, owner_table, step_weight):
    own_mask = mask_spectrum[0]
    length = own_mask.shape[-1]
    slots, _, slab, _ = kernels.shape
    steps = owner_table.shape[0]
    per_core = steps // 2
    devices = groups * tiles
    sub = slab // (groups // 2)
    quarter = length // RADIX

    core_bit, x_bit, y_bit, low_bit = tiles, 2 * tiles, 1, 2
    high_bits = [bit for bit in (2**k for k in range(2, 10)) if bit < tiles]
    bits = {"x": [x_bit], "y": [y_bit], "l": [low_bit], "h": high_bits}

    def exchange(value, flips):
        pairs = [(i, i ^ flips[(i // tiles) % 2]) for i in range(devices)]
        return lax.ppermute(value, ("kgrp", "tile"), pairs)

    received = exchange(kernels, (core_bit, core_bit))
    other_mask = exchange(own_mask, (core_bit, core_bit))
    local_rows, flags, *here = stage(owner_table, kernels, per_core)

    def flag(row):
        return flags[row, 0][None, None] > 0.5

    parted = []
    for step in range(per_core):
        row = 1 + step * slots
        other = received[0]
        for j in range(1, slots):
            other = jnp.where(flag(row + j), received[j], other)
        chip = jnp.where(flag(row), local_rows[step], other)
        low, high = chip[:, :sub], chip[:, sub:]
        parted.append((jnp.where(flag(0), low, high), jnp.where(flag(0), high, low)))
    parted = lax.optimization_barrier(parted)
    values = []
    for step, (give, keep) in enumerate(parted):
        got = exchange(give, (x_bit, x_bit))
        values.append(jnp.where(here[step][0][None, None] > 0.5, keep, got))

    orders = [[[bit for letter in o for bit in bits[letter]] for o in order] for _, order in PIECES]
    rounds = len(orders[0][0])
    team = {}
    for i, ((step, _, _), _) in enumerate(PIECES):
        team.setdefault(step, []).append(i)
    current = {members[0]: values[step][None] for step, members in team.items()}
    pieces = [None] * len(PIECES)

    def split(step):
        whole = current[team[step][0]]
        for i in team[step]:
            _, first, count = PIECES[i][0]
            current[i] = whole[..., first * quarter : (first + count) * quarter]

    for r in range(rounds):
        for step, members in team.items():
            if r == SHARED[step]:
                split(step)
            for i in members[: 1 if r < SHARED[step] else None]:
                got = exchange(current[i], (orders[i][0][r], orders[i][1][r]))
                if r < rounds - 1:
                    current[i] = jnp.concatenate([current[i], got])
                else:
                    pieces[i] = (current[i], got)
    origins = []
    for order in orders:
        origin = []
        for which in range(2):
            flips = [0]
            for bit in order[which]:
                flips = flips + [f ^ bit for f in flips]
            origin.append(flips)
        origins.append(origin)

    right, left = dft_tables(length)
    tables = (jnp.asarray(right), jnp.asarray(left))
    args = (origins, tiles, step_weight, tables)
    theirs, ours = unit(0, [other_mask, own_mask], pieces, *args)
    theirs, kern = unit(1, [other_mask], pieces, *args, accs=[theirs], keep=True)
    arrived = exchange(theirs, (core_bit, core_bit))
    (ours,) = unit(1, [own_mask], pieces, *args, accs=[ours], kern=kern)
    return finish(ours, arrived, lane_order(length))[None]


def solution(mesh):
    in_specs = (P(("kgrp", "tile"), None, None, None), P("kgrp", None, "tile", None), P(), P())
    out_specs = P(("kgrp", "tile"), None, None)

    def body(*args):
        return local(mesh.shape["kgrp"], mesh.shape["tile"], *args)

    return jax.shard_map(body, mesh=mesh, in_specs=in_specs, out_specs=out_specs, check_vma=False)
```

```python
import functools
import itertools
import math

import jax
import jax.numpy as jnp
import numpy as np
from jax import lax
from jax.experimental import pallas as pl
from jax.experimental.pallas import tpu as pltpu
from jax.sharding import PartitionSpec as P


RADIX = 4
BF16 = jnp.bfloat16
F32 = jnp.float32

PIECES = (
    ((0, 0, 2), ("lhyx", "hyxl")),
    ((0, 2, 2), ("lhxy", "hxly")),
    ((1, 0, 2), ("lyhx", "hyxl")),
    ((1, 2, 2), ("lhxy", "lyxh")),
)
SHARED = (1, 0)


def dft_tables(length):
    quarter = length // RADIX
    inner = np.arange(quarter)[:, None]
    tables = []
    for residue in range(RADIX):
        outer = RADIX * np.arange(quarter)[None, :] + residue
        angle = (inner * outer % length) * (2.0 * math.pi / length)
        cos, sin = np.cos(angle) / math.sqrt(length), np.sin(angle) / math.sqrt(length)
        tables.append(np.block([[cos, sin], [-sin, cos]]))
    table = np.stack(tables).astype(np.float32)
    high = table.astype(jnp.bfloat16)
    low = (table - high.astype(np.float32)).astype(jnp.bfloat16)
    right = np.stack([high, low])
    left = np.concatenate([np.swapaxes(high, -1, -2), np.swapaxes(low, -1, -2)], axis=1)
    return right, np.ascontiguousarray(left)


def lane_order(length):
    quarter = length // RADIX
    row = lax.broadcasted_iota(jnp.int32, (length, length), 0)
    lane = lax.broadcasted_iota(jnp.int32, (length, length), 1)
    return (row == (lane % RADIX) * quarter + lane // RADIX).astype(BF16)


def halves(value):
    high = value.astype(BF16)
    return high, (value - high.astype(F32)).astype(BF16)


def dot(left, right):
    return jnp.dot(left, right, preferred_element_type=F32)


def butterflies(quarters):
    (r0, i0), (r1, i1), (r2, i2), (r3, i3) = quarters
    sr, si, dr, di = r0 + r2, i0 + i2, r0 - r2, i0 - i2
    er, ei, fr, fi = r1 + r3, i1 + i3, r1 - r3, i1 - i3
    return (sr + er, si + ei), (dr - fi, di + fr), (sr - er, si - ei), (dr + fi, di - fr)


def unit_kernel(step, origins, tiles, per_core, n_pieces, n_tiles, has_acc, keep, length, *refs):
    weight_ref, right_ref, left_ref = refs[:3]
    mask_refs, refs = refs[3 : 3 + n_tiles], refs[3 + n_tiles :]
    piece_refs, refs = refs[: 2 * n_pieces], refs[2 * n_pieces :]
    acc_refs, refs = (refs[:n_tiles], refs[n_tiles:]) if has_acc else ((None,) * n_tiles, refs)
    if not n_pieces:
        kern, refs = refs[0], refs[1:]
    out_refs, refs = refs[:n_tiles], refs[n_tiles:]
    if n_pieces:
        kern, refs = refs[0], refs[1:]
    rows, z_ref, cols_hi, cols_lo, sem = refs
    quarter = length // RADIX

    group = lax.axis_index("kgrp")
    core = lax.rem(group, 2)
    me = group * tiles + lax.axis_index("tile")
    slab = length // tiles
    index = 0
    for piece, ((piece_step, first, count), _) in enumerate(PIECES):
        if not n_pieces or piece_step != step:
            continue
        sub = piece_refs[0].shape[-2]
        for part in range(2):
            ref = piece_refs[2 * index + part]
            for unit in range(ref.shape[0]):
                flips = [origins[piece][which][part * ref.shape[0] + unit] for which in range(2)]
                flip = flips[0] if flips[0] == flips[1] else jnp.where(core == 0, flips[0], flips[1])
                source = jnp.bitwise_xor(me, flip)
                row = jnp.bitwise_and(source, tiles - 1) * slab
                row = row + lax.shift_right_logical(source, (2 * tiles).bit_length() - 1) * sub
                to = kern.at[:, pl.ds(pl.multiple_of(row, 8), sub), pl.ds(first * quarter, count * quarter)]
                pltpu.make_async_copy(ref.at[unit], to, sem).start()
        index += 1
    if n_pieces:
        pltpu.make_async_copy(kern, kern, sem).wait()

    block, chunk = 128, 16
    slots = rows.shape[0]
    weight = weight_ref[core * per_core + step]

    def fill_rows(tile, b, base):
        at = pl.ds(b * block + base, chunk)
        quarters = []
        for j in range(RADIX):
            lanes = pl.ds(j * quarter, quarter)
            mr, mi = mask_refs[tile][0, at, lanes], mask_refs[tile][1, at, lanes]
            kr, ki = kern[0, at, lanes], kern[1, at, lanes]
            quarters.append((mr * kr - mi * ki, mr * ki + mi * kr))
        for r, pair in enumerate(butterflies(quarters)):
            for part, value in enumerate(pair):
                high, low = halves(value)
                lanes = pl.ds(part * quarter, quarter)
                rows[b % slots, r, pl.ds(base, chunk), lanes] = high
                rows[b % slots, r, pl.ds(block + base, chunk), lanes] = low

    def along_rows(b, r):
        both = dot(rows[b % slots, r], right_ref[0, r])
        rest = dot(rows[b % slots, r, :block], right_ref[1, r])
        z_ref[r, pl.ds(b * block, block), :] = both[:block] + both[block:] + rest

    def fill_cols(r, base):
        quarters = []
        for j in range(RADIX):
            at = pl.ds(j * quarter + base, chunk)
            quarters.append((z_ref[r, at, :quarter], z_ref[r, at, quarter:]))
        for rho, pair in enumerate(butterflies(quarters)):
            for part, value in enumerate(pair):
                at, lanes = pl.ds(part * quarter + base, chunk), pl.ds(r * quarter, quarter)
                cols_hi[rho, at, lanes], cols_lo[rho, at, lanes] = halves(value)

    def along_cols(tile, pair, rho):
        lanes = pl.ds(pair * 2 * quarter, 2 * quarter)
        both = dot(left_ref[rho], cols_hi[rho, :, lanes])
        rest = dot(left_ref[rho, : 2 * quarter], cols_lo[rho, :, lanes])
        field = both[: 2 * quarter] + both[2 * quarter :] + rest
        re, im = field[:quarter], field[quarter:]
        value = weight * (re * re + im * im)
        if has_acc:
            value = value + acc_refs[tile][rho, :, lanes]
        out_refs[tile][rho, :, lanes] = value

    def tasks(function, *lists):
        return [functools.partial(function, *args) for args in itertools.product(*lists)]

    def mix(matmuls, fills):
        count = max(len(matmuls), 1)
        for index in range(count):
            for task in matmuls[index : index + 1]:
                task()
            for task in fills[index * len(fills) // count : (index + 1) * len(fills) // count]:
                task()

    bases, quads = range(0, block, chunk), range(RADIX)
    blocks = range(length // block)
    ahead = range(0, quarter, chunk)
    now, later = (quads[:2], quads[2:]) if slots == len(blocks) else (quads, ())
    mix([], tasks(fill_rows, [0], [0], bases))
    for tile in range(n_tiles):
        for b in blocks[:-1]:
            mix(tasks(along_rows, [b], now), tasks(fill_rows, [tile], [b + 1], bases))
        mix(tasks(along_rows, blocks[-1:], now), [])
        mix(tasks(along_rows, blocks, later), tasks(fill_cols, [0, 1], ahead))
        mix(tasks(along_cols, [tile], [0], quads), tasks(fill_cols, [2, 3], ahead))
        following = tasks(fill_rows, [tile + 1], [0], bases) if tile + 1 < n_tiles else []
        mix(tasks(along_cols, [tile], [1], quads), following)


def unit(step, masks, pieces, origins, tiles, weights, tables, accs=(), kern=None, keep=False):
    length = masks[0].shape[-1]
    used = [pair for pair, (part, _) in zip(pieces, PIECES) if kern is None and part[0] == step]
    flat = [ref for pair in used for ref in pair]
    quarter = length // RADIX
    vmem = pl.BlockSpec(memory_space=pltpu.VMEM)
    hbm = pl.BlockSpec(memory_space=pltpu.HBM)
    smem = pl.BlockSpec(memory_space=pltpu.SMEM)
    n = len(masks)
    late = list(accs) + ([] if kern is None else [kern])
    whole = jax.ShapeDtypeStruct((2, length, length), F32)
    scratch = [
        pltpu.VMEM((2 if n > 1 else length // 128, RADIX, 256, 2 * quarter), BF16),
        pltpu.VMEM((RADIX, length, 2 * quarter), F32),
        pltpu.VMEM((RADIX, 2 * quarter, length), BF16),
        pltpu.VMEM((RADIX, 2 * quarter, length), BF16),
        pltpu.SemaphoreType.DMA,
    ]
    if used and not keep:
        scratch = [pltpu.VMEM(whole.shape, F32)] + scratch
    return pl.pallas_call(
        functools.partial(
            unit_kernel, step, origins, tiles, weights.shape[0] // 2, len(used), n, bool(accs), keep, length
        ),
        out_shape=[jax.ShapeDtypeStruct((RADIX, quarter, length), F32)] * n + [whole] * keep,
        in_specs=[smem, vmem, vmem] + [vmem] * n + [hbm] * len(flat) + [vmem] * len(late),
        out_specs=[vmem] * (n + keep),
        scratch_shapes=scratch,
        compiler_params=pltpu.CompilerParams(vmem_limit_bytes=12 * 2**20),
        cost_estimate=pl.CostEstimate(flops=n * 3 * 2**30, bytes_accessed=8 * 2**20, transcendentals=0),
    )(weights, *tables, *masks, *flat, *late)


def stage_kernel(per_core, owner_ref, kernels_ref, local_ref, flags_ref, *here_refs):
    slots = kernels_ref.shape[0]
    group = lax.axis_index("kgrp")
    core, xpos = lax.rem(group, 2), group // 2
    flags = [xpos == 1]
    for step in range(per_core):
        kernel = owner_ref[core * per_core + step]
        owner, slot = kernel // slots, lax.rem(kernel, slots)
        local_ref[step] = kernels_ref[slot]
        flags += [lax.rem(owner, 2) == core] + [slot == j for j in range(1, slots)]
        here = jnp.where(owner // 2 == xpos, 1.0, 0.0)
        here_refs[step][...] = jnp.full(here_refs[step].shape, here, F32)
    for row, flag in enumerate(flags):
        flags_ref[row] = jnp.full(flags_ref.shape[1:], jnp.where(flag, 1.0, 0.0), F32)


def stage(owner_table, kernels, per_core):
    slots, parts, slab, length = kernels.shape
    vmem = pl.BlockSpec(memory_space=pltpu.VMEM)
    return pl.pallas_call(
        functools.partial(stage_kernel, per_core),
        out_shape=[
            jax.ShapeDtypeStruct((per_core, parts, slab, length), F32),
            jax.ShapeDtypeStruct((1 + per_core * slots, 8, length), F32),
        ]
        + [jax.ShapeDtypeStruct((8, length), F32)] * per_core,
        in_specs=[pl.BlockSpec(memory_space=pltpu.SMEM), vmem],
        out_specs=[vmem] * (2 + per_core),
        compiler_params=pltpu.CompilerParams(vmem_limit_bytes=4 * 2**20),
        name="stage",
    )(owner_table, kernels)


def finish_kernel(a_ref, b_ref, order_ref, out_ref, both, split, sem):
    quarter, _ = a_ref.shape[1:]
    for rho in range(RADIX):
        high, low = halves(a_ref[rho] + b_ref[rho])
        both[0, pl.ds(rho * quarter, quarter), :] = high
        both[1, pl.ds(rho * quarter, quarter), :] = low
    copies = []
    for q in range(0, RADIX, 2):
        lanes = slice(q * quarter, (q + 2) * quarter)
        value = dot(both[0], order_ref[:, lanes]) + dot(both[1], order_ref[:, lanes])
        for k in range(2):
            for rho in range(RADIX):
                rows = slice(rho * quarter, (rho + 1) * quarter)
                split[q + k, pl.ds(rho, quarter, stride=RADIX), :] = value[rows, k * quarter : (k + 1) * quarter]
            to = out_ref.at[:, pl.ds((q + k) * quarter, quarter)]
            copies.append(pltpu.make_async_copy(split.at[q + k], to, sem.at[q + k]))
            copies[-1].start()
    for copy in copies:
        copy.wait()


def finish(mine, other, order):
    _, quarter, length = mine.shape
    vmem = pl.BlockSpec(memory_space=pltpu.VMEM)
    return pl.pallas_call(
        finish_kernel,
        out_shape=jax.ShapeDtypeStruct((length, length), F32),
        in_specs=[vmem] * 3,
        out_specs=pl.BlockSpec(memory_space=pltpu.HBM),
        scratch_shapes=[
            pltpu.VMEM((2, length, length), BF16),
            pltpu.VMEM((RADIX, length, quarter), F32),
            pltpu.SemaphoreType.DMA((RADIX,)),
        ],
        compiler_params=pltpu.CompilerParams(vmem_limit_bytes=8 * 2**20),
        cost_estimate=pl.CostEstimate(flops=2**28, bytes_accessed=3 * 2**20, transcendentals=0),
        name="finish",
    )(mine, other, order)


def local(groups, tiles, mask_spectrum, kernels, owner_table, step_weight):
    own_mask = mask_spectrum[0]
    length = own_mask.shape[-1]
    slots, _, slab, _ = kernels.shape
    steps = owner_table.shape[0]
    per_core = steps // 2
    devices = groups * tiles
    sub = slab // (groups // 2)
    quarter = length // RADIX

    core_bit, x_bit, y_bit, low_bit = tiles, 2 * tiles, 1, 2
    high_bits = [bit for bit in (2**k for k in range(2, 10)) if bit < tiles]
    bits = {"x": [x_bit], "y": [y_bit], "l": [low_bit], "h": high_bits}

    def exchange(value, flips):
        pairs = [(i, i ^ flips[(i // tiles) % 2]) for i in range(devices)]
        return lax.ppermute(value, ("kgrp", "tile"), pairs)

    received = exchange(kernels, (core_bit, core_bit))
    other_mask = exchange(own_mask, (core_bit, core_bit))
    local_rows, flags, *here = stage(owner_table, kernels, per_core)

    def flag(row):
        return flags[row, 0][None, None] > 0.5

    parted = []
    for step in range(per_core):
        row = 1 + step * slots
        other = received[0]
        for j in range(1, slots):
            other = jnp.where(flag(row + j), received[j], other)
        chip = jnp.where(flag(row), local_rows[step], other)
        low, high = chip[:, :sub], chip[:, sub:]
        parted.append((jnp.where(flag(0), low, high), jnp.where(flag(0), high, low)))
    parted = lax.optimization_barrier(parted)
    values = []
    for step, (give, keep) in enumerate(parted):
        got = exchange(give, (x_bit, x_bit))
        values.append(jnp.where(here[step][0][None, None] > 0.5, keep, got))

    orders = [[[bit for letter in o for bit in bits[letter]] for o in order] for _, order in PIECES]
    rounds = len(orders[0][0])
    team = {}
    for i, ((step, _, _), _) in enumerate(PIECES):
        team.setdefault(step, []).append(i)
    current = {members[0]: values[step][None] for step, members in team.items()}
    pieces = [None] * len(PIECES)

    def split(step):
        whole = current[team[step][0]]
        for i in team[step]:
            _, first, count = PIECES[i][0]
            current[i] = whole[..., first * quarter : (first + count) * quarter]

    for r in range(rounds):
        for step, members in team.items():
            if r == SHARED[step]:
                split(step)
            for i in members[: 1 if r < SHARED[step] else None]:
                got = exchange(current[i], (orders[i][0][r], orders[i][1][r]))
                if r < rounds - 1:
                    current[i] = jnp.concatenate([current[i], got])
                else:
                    pieces[i] = (current[i], got)
    origins = []
    for order in orders:
        origin = []
        for which in range(2):
            flips = [0]
            for bit in order[which]:
                flips = flips + [f ^ bit for f in flips]
            origin.append(flips)
        origins.append(origin)

    right, left = dft_tables(length)
    tables = (jnp.asarray(right), jnp.asarray(left))
    args = (origins, tiles, step_weight, tables)
    theirs, ours = unit(0, [other_mask, own_mask], pieces, *args)
    theirs, kern = unit(1, [other_mask], pieces, *args, accs=[theirs], keep=True)
    arrived = exchange(theirs, (core_bit, core_bit))
    (ours,) = unit(1, [own_mask], pieces, *args, accs=[ours], kern=kern)
    return finish(ours, arrived, lane_order(length))[None]


def solution(mesh):
    in_specs = (P(("kgrp", "tile"), None, None, None), P("kgrp", None, "tile", None), P(), P())
    out_specs = P(("kgrp", "tile"), None, None)

    def body(*args):
        return local(mesh.shape["kgrp"], mesh.shape["tile"], *args)

    return jax.shard_map(body, mesh=mesh, in_specs=in_specs, out_specs=out_specs, check_vma=False)
```
